16 devices in a mesh: nodes: 16 (over z, y, x, core).
Axes of the slice: x: 2, y: 2, z: 2, core: 2. Of those that a mesh axis runs over, the one named last changes fastest.
Arguments:
- adjacency: bfloat16 [16384, 16384], P('nodes')
- features: bfloat16 [16384, 100], P('nodes')
- w_hidden: float32 [100, 256], replicated
- w_output: float32 [256, 47], replicated
- labels: int32 [16384], P('nodes')
- train_mask: int32 [16384], P('nodes')
- block_mask: int32 [16, 16], replicated
Outputs:
- output 1: float32 [], replicated
- output 2: float32 [100, 256], replicated
- output 3: float32 [256, 47], replicated
All inputs are finite; a program needn't handle non-finite values.
Results may differ from the reference program's by a relative error of at most 0.001.
Values are sent between devices in bfloat16 or wider.
A program may use at most 1 GiB of HBM per device.

```python
import jax
import jax.numpy as jnp
from jax import lax

NUM_NODES = 16384
BLOCKS = 16
F_IN = 100
HID = 256
CLASSES = 47
EDGE_PERCENT = 15
BLOCK_ROWS = NUM_NODES // BLOCKS


def setup_inputs(seed: int = 0) -> dict:
    keys = jax.random.split(jax.random.key(seed), 9)
    thresholds = jax.random.randint(keys[0], (BLOCKS, 1), BLOCKS // 8, BLOCKS + 1, dtype=jnp.int32)
    block_draw = jax.random.randint(keys[1], (BLOCKS, BLOCKS), 0, BLOCKS, dtype=jnp.int32)
    block_mask = jnp.maximum((block_draw < thresholds).astype(jnp.int32), jnp.eye(BLOCKS, dtype=jnp.int32))
    col_ids = jnp.arange(NUM_NODES, dtype=jnp.int32)

    def edge_rows(block_id):
        edge_draw = jax.random.randint(jax.random.fold_in(keys[2], block_id), (BLOCK_ROWS, NUM_NODES), 0, 100, dtype=jnp.int32)
        row_ids = block_id * BLOCK_ROWS + jnp.arange(BLOCK_ROWS, dtype=jnp.int32)
        col_keep = jnp.repeat(block_mask[block_id], BLOCK_ROWS) > 0
        edge_on = ((edge_draw < EDGE_PERCENT) | (row_ids[:, None] == col_ids[None, :])) & col_keep[None, :]
        raw_weight = edge_on.astype(jnp.float32)
        return (raw_weight / jnp.sum(raw_weight, axis=1, keepdims=True)).astype(jnp.bfloat16)

    adjacency = lax.map(edge_rows, jnp.arange(BLOCKS, dtype=jnp.int32)).reshape(NUM_NODES, NUM_NODES)
    centers = jax.random.normal(keys[3], (BLOCKS, F_IN), jnp.float32)
    noise = jax.random.normal(keys[4], (NUM_NODES, F_IN), jnp.float32)
    features = (jnp.repeat(centers, BLOCK_ROWS, axis=0) + noise).astype(jnp.bfloat16)
    w_hidden = jax.random.normal(keys[5], (F_IN, HID), jnp.float32) * (F_IN ** -0.5 * BLOCKS ** 0.25)
    w_output = jax.random.normal(keys[6], (HID, CLASSES), jnp.float32) * (2.0 * HID ** -0.5)
    labels = jax.random.randint(keys[7], (NUM_NODES,), 0, CLASSES, dtype=jnp.int32)
    label_draw = jax.random.randint(keys[8], (NUM_NODES,), 0, 100, dtype=jnp.int32)
    train_mask = jnp.maximum((label_draw < 40).astype(jnp.int32), (col_ids == 0).astype(jnp.int32))
    return dict(adjacency=adjacency, features=features, w_hidden=w_hidden, w_output=w_output, labels=labels, train_mask=train_mask, block_mask=block_mask)


def masked_product(adj_blocks, block_mask, values):
    width = values.shape[-1]
    value_blocks = values.reshape(BLOCKS, BLOCK_ROWS, width)

    def one_block(block_item):
        adj_rows, mask_row = block_item
        scaled = value_blocks * mask_row.astype(values.dtype)[:, None, None]
        return jnp.dot(adj_rows, scaled.reshape(NUM_NODES, width), preferred_element_type=jnp.float32)

    return lax.map(one_block, (adj_blocks, block_mask)).reshape(NUM_NODES, width)


def masked_transpose_product(adj_blocks, block_mask, grads):
    width = grads.shape[-1]
    grad_blocks = grads.reshape(BLOCKS, BLOCK_ROWS, width)

    def add_block(running_sum, block_item):
        adj_rows, mask_row, grad_rows = block_item
        contrib = jnp.dot(adj_rows.T, grad_rows, preferred_element_type=jnp.float32)
        contrib = contrib.reshape(BLOCKS, BLOCK_ROWS, width) * mask_row.astype(jnp.float32)[:, None, None]
        return running_sum + contrib.reshape(NUM_NODES, width), None

    start_sum = jnp.zeros((NUM_NODES, width), jnp.float32)
    total_sum, _ = lax.scan(add_block, start_sum, (adj_blocks, block_mask, grad_blocks))
    return total_sum


def reference(adjacency, features, w_hidden, w_output, labels, train_mask, block_mask):
    adj_blocks = adjacency.reshape(BLOCKS, BLOCK_ROWS, NUM_NODES)
    w_hidden_bf = w_hidden.astype(jnp.bfloat16)
    w_output_bf = w_output.astype(jnp.bfloat16)
    proj_one = jnp.dot(features, w_hidden_bf, preferred_element_type=jnp.float32).astype(jnp.bfloat16)
    agg_one = masked_product(adj_blocks, block_mask, proj_one)
    hidden = jnp.maximum(agg_one, 0.0).astype(jnp.bfloat16)
    proj_two = jnp.dot(hidden, w_output_bf, preferred_element_type=jnp.float32).astype(jnp.bfloat16)
    logits = masked_product(adj_blocks, block_mask, proj_two)
    label_weight = train_mask.astype(jnp.float32)
    label_count = jnp.sum(label_weight)
    log_norm = jax.nn.logsumexp(logits, axis=-1)
    one_hot = (labels[:, None] == jnp.arange(CLASSES)[None, :]).astype(jnp.float32)
    picked = jnp.sum(logits * one_hot, axis=-1)
    mean_loss = jnp.sum(label_weight * (log_norm - picked)) / label_count
    probabilities = jnp.exp(logits - log_norm[:, None])
    grad_logits = ((probabilities - one_hot) * (label_weight / label_count)[:, None]).astype(jnp.bfloat16)
    grad_proj_two = masked_transpose_product(adj_blocks, block_mask, grad_logits).astype(jnp.bfloat16)
    grad_w_output = jnp.dot(hidden.T, grad_proj_two, preferred_element_type=jnp.float32)
    grad_hidden = jnp.dot(grad_proj_two, w_output_bf.T, preferred_element_type=jnp.float32)
    grad_agg = jnp.where(agg_one > 0, grad_hidden, 0.0).astype(jnp.bfloat16)
    grad_proj_one = masked_transpose_product(adj_blocks, block_mask, grad_agg).astype(jnp.bfloat16)
    grad_w_hidden = jnp.dot(features.T, grad_proj_one, preferred_element_type=jnp.float32)
    return (mean_loss, grad_w_hidden, grad_w_output)
```

```python
import functools

import jax
import jax.numpy as jnp
from jax import lax
from jax.experimental import pallas as pl
from jax.experimental.pallas import tpu as pltpu
from jax.sharding import PartitionSpec as P

AXIS = 'nodes'
MESH = pl.DeviceIdType.MESH
F32, BF16 = jnp.float32, jnp.bfloat16
LAST = (((1,), (1,)), ((), ()))
NB, BR, FI, HID, NC, CP = 16, 1024, 100, 256, 47, 48
X, Y, Z = 1, 2, 4
DIMS = (X, Y, Z)
NEXT = {X: Y, Y: Z, Z: X}
PREV = {Y: X, Z: Y, X: Z}
XYZ = X + Y + Z
LOSS_LANE = 64

ORDER = [(0, 0), (0, 1)]
for group in ((X, Y, Z), (X + Y, Y + Z, Z + X), (XYZ,)):
    ORDER += [(q, 0) for q in group] + [(q, 1) for q in group]
SLOT = {qc: i for i, qc in enumerate(ORDER)}

AG_COPIES, RS_COPIES = 17, 29
AG_X, AG_Y = 0, AG_COPIES
RS_D2, RS_D1 = 2 * AG_COPIES, 2 * AG_COPIES + RS_COPIES
AR = 2 * AG_COPIES + 2 * RS_COPIES
N_SEM = AR + 30


def peer(me, mask):
    out = me
    for k in range(4):
        if mask >> k & 1:
            out = out + (1 - 2 * (me // (1 << k) % 2)) * (1 << k)
    return out


def kernel(a_hbm, x_hbm, wh_ref, wo_ref, lab_ref, tm_ref,
           loss_ref, gwh_ref, gwo_ref,
           a_v, xg, yg, z1, hid, pos, z2, r2, ra2, rb2, rc2, r1, ra1, rb1, rc1, stage, wop,
           fsrc, frecv, fsum, fall, a_sem, x_sem, send_sem, recv_sem):
    me = lax.axis_index(AXIS)
    devs = {m: peer(me, m) for m in range(16)}

    def rcopy(src, dst, k, mask):
        return pltpu.make_async_remote_copy(
            src_ref=src, dst_ref=dst, send_sem=send_sem.at[k], recv_sem=recv_sem.at[k],
            device_id=(devs[mask],), device_id_type=MESH)

    a_copies = []
    for s, (q, c) in enumerate(ORDER):
        col = pl.multiple_of(devs[2 * q + c] * BR, BR)
        a_copies.append(pltpu.make_async_copy(a_hbm.at[:, pl.ds(col, BR)], a_v.at[s], a_sem.at[s]))
    x_copy = pltpu.make_async_copy(x_hbm, xg.at[0], x_sem)
    x_copy.start()
    for cp in a_copies:
        cp.start()

    barrier = pltpu.get_barrier_semaphore()
    for m in range(1, 16):
        pl.semaphore_signal(barrier, inc=1, device_id=(devs[m],), device_id_type=MESH)
    wop[...] = jnp.zeros_like(wop)
    wop[:, :NC] = wo_ref[...].astype(BF16)
    fsrc[...] = jnp.zeros_like(fsrc)
    z2[...] = jnp.zeros_like(z2)
    z1[...] = jnp.zeros_like(z1)
    pl.semaphore_wait(barrier, 15)
    x_copy.wait()

    sent = []

    def start(cp):
        cp.start()
        sent.append(cp)
        return cp

    def gather(base, g, pieces, work):
        def core_fwd(q):
            return start(rcopy(g.at[SLOT[q, 0]], g.at[SLOT[q, 1]], base + 9 + q, 1))

        one = {d: start(rcopy(g.at[0], g.at[SLOT[d, 0]], base + i, 2 * d)) for i, d in enumerate(DIMS)}
        half = {0: core_fwd(0)}
        work(0, 1)
        half[0].wait_recv()
        work(1, 2)
        two, three = {}, {}
        for d in DIMS:
            one[d].wait_recv()
        for i, d in enumerate(DIMS):
            e = NEXT[d]
            two[d] = start(rcopy(g.at[SLOT[e, 0]], g.at[SLOT[d + e, 0]], base + 3 + i, 2 * d))
        for d in DIMS:
            half[d] = core_fwd(d)
        work(2, 5)
        for d in DIMS:
            half[d].wait_recv()
        work(5, 8)
        for d in DIMS:
            two[d].wait_recv()
        for i, d in enumerate(DIMS):
            rows = pl.ds(*pieces[i])
            three[d] = start(rcopy(g.at[SLOT[XYZ - d, 0], rows], g.at[SLOT[XYZ, 0], rows], base + 6 + i, 2 * d))
        for d in DIMS:
            half[XYZ - d] = core_fwd(XYZ - d)
        work(8, 11)
        for d in DIMS:
            half[XYZ - d].wait_recv()
        work(11, 14)
        for d in DIMS:
            three[d].wait_recv()
        half[XYZ] = core_fwd(XYZ)
        work(14, 15)
        half[XYZ].wait_recv()
        work(15, 16)

    wh = wh_ref[...].astype(BF16)

    def layer_one(lo, hi):
        for s in range(lo, hi):
            a_copies[s].wait()

        def body(s, carry):
            hid[...] = jnp.dot(xg[s], wh, preferred_element_type=F32).astype(BF16)
            z1[...] += jnp.dot(a_v[s], hid[...], preferred_element_type=F32)
            return carry

        lax.fori_loop(lo, hi, body, 0)

    gather(AG_X, xg, ((0, 352), (352, 336), (688, 336)), layer_one)

    hid[...] = jnp.maximum(z1[...], 0.0).astype(BF16)
    tm = tm_ref[...].astype(F32)
    y2t = jnp.transpose(jnp.dot(hid[...], wop[...], preferred_element_type=F32))[:CP]
    row = lax.broadcasted_iota(jnp.int32, (CP, BR), 0)
    yg[0] = jnp.where(row == NC, tm, y2t).astype(BF16)

    first = [True]

    def layer_two(lo, hi):
        def body(s, carry):
            z2[:, :CP] += lax.dot_general(a_v[s], yg[s], LAST, preferred_element_type=F32)
            return carry

        lax.fori_loop(lo, hi, body, 0)
        if first[0]:
            first[0] = False
            pos[...] = jnp.where(jnp.transpose(z1[...]) > 0, 1.0, 0.0).astype(BF16)

    gather(AG_Y, yg, ((0, 16), (16, 16), (32, 16)), layer_two)

    count = jnp.zeros((1, BR), F32)
    for s in range(NB):
        count = count + yg[s, NC:CP, :].astype(F32)
    total = jnp.sum(count, axis=1, keepdims=True)
    zt = jnp.transpose(z2[...])[:CP]
    valid = row < NC
    top = jnp.max(jnp.where(valid, zt, -jnp.inf), axis=0, keepdims=True)
    lse = top + jnp.log(jnp.sum(jnp.where(valid, jnp.exp(zt - top), 0.0), axis=0, keepdims=True))
    hot = row == lab_ref[...]
    picked = jnp.sum(jnp.where(hot, zt, 0.0), axis=0, keepdims=True)
    loss = jnp.sum(tm * (lse - picked), axis=1, keepdims=True)
    grad = (jnp.exp(zt - lse) - hot.astype(F32)) * (tm / total)
    gt = jnp.where(valid, grad, 0.0).astype(BF16)

    def scatter(base, r, ra, rb, rc, pieces, left, stages, early):
        def rows(i):
            return pl.ds(*pieces[i])

        pair = {}

        def produce(k, q):
            st = stages(k)
            if not early and k >= 2:
                pair[k - 2].wait_send()
                sent[:] = [cp for cp in sent if cp is not pair[k - 2]]
            st[...] = jnp.dot(left, a_v[SLOT[q, 1]], preferred_element_type=F32)
            pair[k] = start(rcopy(st, r.at[q], base + k, 1))
            own = jnp.dot(left, a_v[SLOT[q, 0]], preferred_element_type=F32)
            pair[k].wait_recv()
            r[q] = r[q] + own

        def send(q, i, dst, k, d):
            return start(rcopy(r.at[q, rows(i)], dst, k, 2 * d))

        three, two, one = {}, {}, {}
        produce(0, XYZ)
        for i, d in enumerate(DIMS):
            three[d] = send(XYZ, i, ra.at[rows(i)], base + 8 + i, d)
        for k, d in enumerate(DIMS):
            q = d + NEXT[d]
            produce(1 + k, q)
            for i, e in enumerate(DIMS):
                if e + q != XYZ:
                    two[d, i] = send(q, i, rb.at[k, rows(i)], base + 11 + 3 * k + i, d)

        def outer():
            for i, e in enumerate(DIMS):
                three[e].wait_recv()
                q = XYZ - e
                r[q, rows(i)] = r[q, rows(i)] + ra[rows(i)]
                d = NEXT[e]
                k = DIMS.index(d)
                two[d, i] = send(q, i, rb.at[k, rows(i)], base + 11 + 3 * k + i, d)

        def inner():
            for j in range(3):
                for n, e in enumerate(DIMS):
                    d = PREV[e]
                    k = DIMS.index(d)
                    last = DIMS.index(XYZ - d - NEXT[d])
                    i = (last + 1 + j) % 3
                    two[d, i].wait_recv()
                    r[e, rows(i)] = r[e, rows(i)] + rb[k, rows(i)]
                    one[e, i] = send(e, i, rc.at[n, rows(i)], base + 20 + 3 * n + i, e)

        if early:
            outer()
        for k, d in enumerate(DIMS):
            produce(4 + k, d)
        if early:
            inner()
            produce(7, 0)
        else:
            produce(7, 0)
            outer()
            inner()
        for j in range(3):
            for n, e in enumerate(DIMS):
                i = (DIMS.index(XYZ - PREV[e] - e) + 1 + j) % 3
                one[e, i].wait_recv()
                r[0, rows(i)] = r[0, rows(i)] + rc[n, rows(i)]

    def stage_d2(k):
        return stage.at[k // 4, pl.ds(CP * (k % 4), CP)]

    scatter(RS_D2, r2, ra2, rb2, rc2, ((0, 16), (16, 16), (32, 16)), gt, stage_d2, True)

    d2t = r2[0].astype(BF16)
    for cp in sent:
        cp.wait_send()
    sent.clear()
    grad_hid = jnp.dot(wop[:, :CP], d2t, preferred_element_type=F32)
    pos[...] = jnp.where(pos[...] > 0, grad_hid, 0.0).astype(BF16)
    gwo_t = jnp.dot(d2t, hid[...], preferred_element_type=F32)
    gwo = jnp.transpose(jnp.concatenate([gwo_t, jnp.zeros((128 - CP, HID), F32)], axis=0))
    lane = lax.broadcasted_iota(jnp.int32, (HID, 128), 1)
    gwo = jnp.where(lane == LOSS_LANE, loss, gwo)
    for i in range(NB):
        fsrc[i, 16:32, :] = gwo[16 * i:16 * i + 16]

    def stage_d1(k):
        return stage.at[k % 2]

    scatter(RS_D1, r1, ra1, rb1, rc1, ((0, 88), (88, 88), (176, 80)), pos[...], stage_d1, False)

    d1t = r1[0].astype(BF16)
    gwh_t = jnp.dot(d1t, xg[0], preferred_element_type=F32)
    for i in range(NB):
        fsrc[i, 0:16, 0:FI] = gwh_t[16 * i:16 * i + 16]
    out_copies = [start(rcopy(fsrc.at[devs[m]], frecv.at[m], AR + m - 1, m)) for m in range(1, 16)]
    acc = fsrc[me]
    for m in range(1, 16):
        out_copies[m - 1].wait_recv()
        acc = acc + frecv[m]
    fsum[...] = acc
    fall[me] = acc
    for m in range(1, 16):
        start(rcopy(fsum, fall.at[me], AR + 15 + m - 1, m))
    for m in range(1, 16):
        rcopy(fsum, fall.at[devs[m]], AR + 15 + m - 1, m).wait_recv()
    gwh_all = jnp.concatenate([fall[i, 0:16, :] for i in range(NB)], axis=0)
    gwh_ref[...] = jnp.transpose(gwh_all)[:FI]
    for i in range(NB):
        gwo_ref[16 * i:16 * i + 16, :] = fall[i, 16:32, 0:NC]
    loss_ref[...] = fall[0, 16:17, LOSS_LANE:LOSS_LANE + 1] / total
    for cp in sent:
        cp.wait_send()


def device_step(adj_rows, feat_rows, w_hidden, w_output, labels, train_mask, block_mask):
    del block_mask
    vmem = pl.BlockSpec(memory_space=pltpu.VMEM)
    hbm = pl.BlockSpec(memory_space=pl.ANY)
    loss, gwh, gwo = pl.pallas_call(
        kernel,
        out_shape=(
            jax.ShapeDtypeStruct((1, 1), F32),
            jax.ShapeDtypeStruct((FI, HID), F32),
            jax.ShapeDtypeStruct((HID, NC), F32),
        ),
        in_specs=[hbm, hbm, vmem, vmem, vmem, vmem],
        out_specs=(vmem, vmem, vmem),
        scratch_shapes=[
            pltpu.VMEM((NB, BR, BR), BF16),
            pltpu.VMEM((NB, BR, FI), BF16),
            pltpu.VMEM((NB, CP, BR), BF16),
            pltpu.VMEM((BR, HID), F32),
            pltpu.VMEM((BR, HID), BF16),
            pltpu.VMEM((HID, BR), BF16),
            pltpu.VMEM((BR, 128), F32),
            pltpu.VMEM((8, CP, BR), F32),
            pltpu.VMEM((CP, BR), F32),
            pltpu.VMEM((3, CP, BR), F32),
            pltpu.VMEM((3, CP, BR), F32),
            pltpu.VMEM((8, HID, BR), F32),
            pltpu.VMEM((HID, BR), F32),
            pltpu.VMEM((3, HID, BR), F32),
            pltpu.VMEM((3, HID, BR), F32),
            pltpu.VMEM((2, HID, BR), F32),
            pltpu.VMEM((HID, 128), BF16),
            pltpu.VMEM((NB, 32, 128), F32),
            pltpu.VMEM((NB, 32, 128), F32),
            pltpu.VMEM((32, 128), F32),
            pltpu.VMEM((NB, 32, 128), F32),
            pltpu.SemaphoreType.DMA((NB,)),
            pltpu.SemaphoreType.DMA,
            pltpu.SemaphoreType.DMA((N_SEM,)),
            pltpu.SemaphoreType.DMA((N_SEM,)),
        ],
        compiler_params=pltpu.CompilerParams(
            collective_id=0, has_side_effects=True, vmem_limit_bytes=67_043_328),
        name='gcn_step',
    )(adj_rows, feat_rows, w_hidden, w_output, labels.reshape(1, -1), train_mask.reshape(1, -1))
    return loss[0, 0], gwh, gwo


def solution(mesh):
    row_spec = P(AXIS, None)
    vec_spec = P(AXIS)
    return jax.shard_map(
        device_step, mesh=mesh,
        in_specs=(row_spec, row_spec, P(), P(), vec_spec, vec_spec, P()),
        out_specs=(P(), P(), P()), check_vma=False)
```

```python
import functools

import jax
import jax.numpy as jnp
from jax import lax
from jax.experimental import pallas as pl
from jax.experimental.pallas import tpu as pltpu
from jax.sharding import PartitionSpec as P

AXIS = 'nodes'
MESH = pl.DeviceIdType.MESH
F32, BF16 = jnp.float32, jnp.bfloat16
FIRST = (((0,), (0,)), ((), ()))
LAST = (((1,), (1,)), ((), ()))
NB, BR, FI, HID, NC, CP = 16, 1024, 100, 256, 47, 48
X, Y, Z = 1, 2, 4
DIMS = (X, Y, Z)
NEXT = {X: Y, Y: Z, Z: X}
PREV = {Y: X, Z: Y, X: Z}
XYZ = X + Y + Z
LOSS_LANE = 64

ORDER = [(0, 0), (0, 1)]
for group in ((X, Y, Z), (X + Y, Y + Z, Z + X), (XYZ,)):
    ORDER += [(q, 0) for q in group] + [(q, 1) for q in group]
SLOT = {qc: i for i, qc in enumerate(ORDER)}

AG_COPIES, RS_COPIES = 17, 29
AG_X, AG_Y = 0, AG_COPIES
RS_D2, RS_D1 = 2 * AG_COPIES, 2 * AG_COPIES + RS_COPIES
AR = 2 * AG_COPIES + 2 * RS_COPIES
N_SEM = AR + 30


def peer(me, mask):
    out = me
    for k in range(4):
        if mask >> k & 1:
            out = out + (1 - 2 * (me // (1 << k) % 2)) * (1 << k)
    return out


def kernel(a_hbm, x_hbm, wh_ref, wo_ref, lab_ref, tm_ref,
           sums_ref, count_ref,
           a_v, xg, yg, y1, z1, hid, pos, z2, r2, ra2, rb2, rc2, r1, ra1, rb1, rc1, stage, wop,
           fsrc, frecv, fsum, fall, a_sem, x_sem, send_sem, recv_sem):
    me = lax.axis_index(AXIS)
    devs = {m: peer(me, m) for m in range(16)}

    def rcopy(src, dst, k, mask):
        return pltpu.make_async_remote_copy(
            src_ref=src, dst_ref=dst, send_sem=send_sem.at[k], recv_sem=recv_sem.at[k],
            device_id=(devs[mask],), device_id_type=MESH)

    a_copies = []
    for s, (q, c) in enumerate(ORDER):
        col = pl.multiple_of(devs[2 * q + c] * BR, BR)
        a_copies.append(pltpu.make_async_copy(a_hbm.at[:, pl.ds(col, BR)], a_v.at[s], a_sem.at[s]))
    x_copy = pltpu.make_async_copy(x_hbm, xg.at[0], x_sem)
    x_copy.start()
    for cp in a_copies:
        cp.start()

    barrier = pltpu.get_barrier_semaphore()
    for m in (1, 2, 4, 8):
        pl.semaphore_signal(barrier, inc=1, device_id=(devs[m],), device_id_type=MESH)
    wop[...] = jnp.zeros_like(wop)
    wop[:NC] = wo_ref[...].astype(BF16)
    fsrc[...] = jnp.zeros_like(fsrc)
    z2[...] = jnp.zeros_like(z2)
    z1[...] = jnp.zeros_like(z1)
    pl.semaphore_wait(barrier, 4)
    x_copy.wait()

    sent = []

    def start(cp):
        cp.start()
        sent.append(cp)
        return cp

    def gather(base, g, pieces, work, early):
        def core_fwd(q):
            return start(rcopy(g.at[SLOT[q, 0]], g.at[SLOT[q, 1]], base + 9 + q, 1))

        one = {d: start(rcopy(g.at[0], g.at[SLOT[d, 0]], base + i, 2 * d)) for i, d in enumerate(DIMS)}
        half = {0: core_fwd(0)}
        two, three = {}, {}
        for n in range(early):
            work(n, n + 1)
            if n == 0:
                half[0].wait_recv()
        for i, d in enumerate(DIMS):
            e = NEXT[d]
            one[e].wait_recv()
            two[d] = start(rcopy(g.at[SLOT[e, 0]], g.at[SLOT[d + e, 0]], base + 3 + i, 2 * d))
        for d in DIMS:
            half[d] = core_fwd(d)
        if not early:
            half[0].wait_recv()
            work(0, 2)
        work(2, 5)
        for d in DIMS:
            half[d].wait_recv()
        work(5, 8)
        for d in DIMS:
            two[d].wait_recv()
        for i, d in enumerate(DIMS):
            rows = pl.ds(*pieces[i])
            three[d] = start(rcopy(g.at[SLOT[XYZ - d, 0], rows], g.at[SLOT[XYZ, 0], rows], base + 6 + i, 2 * d))
        for d in DIMS:
            half[XYZ - d] = core_fwd(XYZ - d)
        work(8, 11)
        for d in DIMS:
            half[XYZ - d].wait_recv()
        work(11, 14)
        for d in DIMS:
            three[d].wait_recv()
        half[XYZ] = core_fwd(XYZ)
        work(14, 15)
        half[XYZ].wait_recv()
        work(15, 16)

    wh = wh_ref[...].astype(BF16)

    def layer_one(lo, hi):
        for s in range(lo, hi):
            a_copies[s].wait()

        def proj(s, ref):
            ref[...] = lax.dot_general(xg[s], wh, FIRST, preferred_element_type=F32).astype(BF16)

        bufs = (hid, y1.at[0], y1.at[1])
        for n, s in enumerate(range(lo, hi)):
            proj(s, bufs[n])
        for n, s in enumerate(range(lo, hi)):
            z1[...] += jnp.dot(a_v[s], bufs[n][...], preferred_element_type=F32)

    gather(AG_X, xg, ((0, 32), (32, 32), (64, 36)), layer_one, 0)

    hid[...] = jnp.maximum(z1[...], 0.0).astype(BF16)
    tm = tm_ref[...].astype(F32)
    y2t = lax.dot_general(wop[...], hid[...], LAST, preferred_element_type=F32)
    row = lax.broadcasted_iota(jnp.int32, (CP, BR), 0)
    yg[0] = jnp.where(row == NC, tm, y2t).astype(BF16)

    first = [True]

    def layer_two(lo, hi):
        def body(s, carry):
            z2[:, :CP] += lax.dot_general(a_v[s], yg[s], LAST, preferred_element_type=F32)
            return carry

        lax.fori_loop(lo, hi, body, 0)
        if first[0]:
            first[0] = False
            pos[...] = jnp.where(jnp.transpose(z1[...]) > 0, 1.0, 0.0).astype(BF16)

    gather(AG_Y, yg, ((0, 16), (16, 16), (32, 16)), layer_two, 2)

    count = jnp.zeros((1, BR), F32)
    for s in range(NB):
        count = count + yg[s, NC:CP, :].astype(F32)
    total = jnp.sum(count, axis=1, keepdims=True)
    zt = jnp.transpose(z2[...])[:CP]
    valid = row < NC
    top = jnp.max(jnp.where(valid, zt, -jnp.inf), axis=0, keepdims=True)
    lse = top + jnp.log(jnp.sum(jnp.where(valid, jnp.exp(zt - top), 0.0), axis=0, keepdims=True))
    hot = row == lab_ref[...]
    picked = jnp.sum(jnp.where(hot, zt, 0.0), axis=0, keepdims=True)
    loss = jnp.sum(tm * (lse - picked), axis=1, keepdims=True)
    grad = (jnp.exp(zt - lse) - hot.astype(F32)) * (tm / total)
    gt = jnp.where(valid, grad, 0.0).astype(BF16)

    def scatter(base, r, ra, rb, rc, pieces, left, stages, early):
        def rows(i):
            return pl.ds(*pieces[i])

        pair = {}

        def other(k, q):
            st = stages(k)
            if not early and k >= 2:
                pair[k - 2].wait_send()
                sent[:] = [cp for cp in sent if cp is not pair[k - 2]]
            st[...] = jnp.dot(left, a_v[SLOT[q, 1]], preferred_element_type=F32)
            pair[k] = start(rcopy(st, r.at[q], base + k, 1))

        def own(k, q):
            pair[k].wait_recv()
            r[q] = r[q] + jnp.dot(left, a_v[SLOT[q, 0]], preferred_element_type=F32)

        def send(q, i, dst, k, d):
            return start(rcopy(r.at[q, rows(i)], dst, k, 2 * d))

        three, two, one = {}, {}, {}
        order = (XYZ,) + tuple(d + NEXT[d] for d in DIMS) + DIMS + (0,)

        def produce(k):
            if k < 7:
                other(k + 1, order[k + 1])
            own(k, order[k])

        other(0, XYZ)
        produce(0)
        for i, d in enumerate(DIMS):
            three[d] = send(XYZ, i, ra.at[rows(i)], base + 8 + i, d)
        for k, d in enumerate(DIMS):
            q = d + NEXT[d]
            produce(1 + k)
            for i, e in enumerate(DIMS):
                if e + q != XYZ:
                    two[d, i] = send(q, i, rb.at[k, rows(i)], base + 11 + 3 * k + i, d)

        def outer():
            for i, e in enumerate(DIMS):
                three[e].wait_recv()
                q = XYZ - e
                r[q, rows(i)] = r[q, rows(i)] + ra[rows(i)]
                d = NEXT[e]
                k = DIMS.index(d)
                two[d, i] = send(q, i, rb.at[k, rows(i)], base + 11 + 3 * k + i, d)

        def inner():
            for j in range(3):
                for n, e in enumerate(DIMS):
                    d = PREV[e]
                    k = DIMS.index(d)
                    last = DIMS.index(XYZ - d - NEXT[d])
                    i = (last + 1 + j) % 3
                    two[d, i].wait_recv()
                    r[e, rows(i)] = r[e, rows(i)] + rb[k, rows(i)]
                    one[e, i] = send(e, i, rc.at[n, rows(i)], base + 20 + 3 * n + i, e)

        if early:
            outer()
        for k, d in enumerate(DIMS):
            produce(4 + k)
        if early:
            inner()
            produce(7)
        else:
            produce(7)
            outer()
            inner()
        for j in range(3):
            for n, e in enumerate(DIMS):
                i = (DIMS.index(XYZ - PREV[e] - e) + 1 + j) % 3
                one[e, i].wait_recv()
                r[0, rows(i)] = r[0, rows(i)] + rc[n, rows(i)]

    def stage_d2(k):
        return stage.at[k // 4, pl.ds(CP * (k % 4), CP)]

    scatter(RS_D2, r2, ra2, rb2, rc2, ((0, 16), (16, 16), (32, 16)), gt, stage_d2, True)

    d2t = r2[0].astype(BF16)
    for cp in sent:
        cp.wait_send()
    sent.clear()
    grad_hid = lax.dot_general(wop[...], d2t, FIRST, preferred_element_type=F32)
    pos[...] = jnp.where(pos[...] > 0, grad_hid, 0.0).astype(BF16)
    gwo_t = jnp.dot(d2t, hid[...], preferred_element_type=F32)
    gwo = jnp.transpose(jnp.concatenate([gwo_t, jnp.zeros((128 - CP, HID), F32)], axis=0))
    lane = lax.broadcasted_iota(jnp.int32, (HID, 128), 1)
    gwo = jnp.where(lane == LOSS_LANE, loss, gwo)
    for i in range(NB):
        fsrc[i, 16:32, :] = gwo[16 * i:16 * i + 16]

    def stage_d1(k):
        return stage.at[k % 2]

    scatter(RS_D1, r1, ra1, rb1, rc1, ((0, 88), (88, 88), (176, 80)), pos[...], stage_d1, False)

    d1t = r1[0].astype(BF16)
    gwh_t = lax.dot_general(d1t, xg[0], LAST, preferred_element_type=F32)
    for i in range(NB):
        fsrc[i, 0:16, 0:FI] = gwh_t[16 * i:16 * i + 16]
    out_copies = [start(rcopy(fsrc.at[devs[m]], frecv.at[m], AR + m - 1, m)) for m in range(1, 16)]
    acc = fsrc[me]
    for m in range(1, 16):
        out_copies[m - 1].wait_recv()
        acc = acc + frecv[m]
    fsum[...] = acc
    fall[me] = acc
    for m in range(1, 16):
        start(rcopy(fsum, fall.at[me], AR + 15 + m - 1, m))
    for m in range(1, 16):
        rcopy(fsum, fall.at[devs[m]], AR + 15 + m - 1, m).wait_recv()
    for i in range(NB):
        sums_ref[i] = fall[i]
    count_ref[...] = total
    for cp in sent:
        cp.wait_send()


def unpack(sums_ref, count_ref, loss_ref, gwh_ref, gwo_ref):
    gwh = jnp.concatenate([sums_ref[i, 0:16, :] for i in range(NB)], axis=0)
    gwo = jnp.concatenate([sums_ref[i, 16:32, :] for i in range(NB)], axis=0)
    gwh_ref[...] = jnp.transpose(gwh)[:FI]
    gwo_ref[...] = jnp.transpose(gwo)[:NC]
    loss_ref[...] = gwo[0:1, LOSS_LANE:LOSS_LANE + 1] / count_ref[...]


def device_step(adj_rows, feat_rows, w_hidden, w_output, labels, train_mask, block_mask):
    del block_mask
    vmem = pl.BlockSpec(memory_space=pltpu.VMEM)
    hbm = pl.BlockSpec(memory_space=pl.ANY)
    sums, count = pl.pallas_call(
        kernel,
        out_shape=(
            jax.ShapeDtypeStruct((NB, 32, 128), F32),
            jax.ShapeDtypeStruct((1, 1), F32),
        ),
        in_specs=[hbm, hbm, vmem, vmem, vmem, vmem],
        out_specs=(vmem, vmem),
        scratch_shapes=[
            pltpu.VMEM((NB, BR, BR), BF16),
            pltpu.VMEM((NB, FI, BR), BF16),
            pltpu.VMEM((NB, CP, BR), BF16),
            pltpu.VMEM((2, BR, HID), BF16),
            pltpu.VMEM((BR, HID), F32),
            pltpu.VMEM((BR, HID), BF16),
            pltpu.VMEM((HID, BR), BF16),
            pltpu.VMEM((BR, 128), F32),
            pltpu.VMEM((8, CP, BR), F32),
            pltpu.VMEM((CP, BR), F32),
            pltpu.VMEM((3, CP, BR), F32),
            pltpu.VMEM((3, CP, BR), F32),
            pltpu.VMEM((8, HID, BR), F32),
            pltpu.VMEM((HID, BR), F32),
            pltpu.VMEM((3, HID, BR), F32),
            pltpu.VMEM((3, HID, BR), F32),
            pltpu.VMEM((2, HID, BR), F32),
            pltpu.VMEM((CP, HID), BF16),
            pltpu.VMEM((NB, 32, 128), F32),
            pltpu.VMEM((NB, 32, 128), F32),
            pltpu.VMEM((32, 128), F32),
            pltpu.VMEM((NB, 32, 128), F32),
            pltpu.SemaphoreType.DMA((NB,)),
            pltpu.SemaphoreType.DMA,
            pltpu.SemaphoreType.DMA((N_SEM,)),
            pltpu.SemaphoreType.DMA((N_SEM,)),
        ],
        compiler_params=pltpu.CompilerParams(
            collective_id=0, has_side_effects=True, vmem_limit_bytes=67_043_328),
        name='gcn_step',
    )(adj_rows, feat_rows.T, w_hidden, w_output.T, labels.reshape(1, -1), train_mask.reshape(1, -1))
    loss, gwh, gwo = pl.pallas_call(
        unpack,
        out_shape=(
            jax.ShapeDtypeStruct((1, 1), F32),
            jax.ShapeDtypeStruct((FI, HID), F32),
            jax.ShapeDtypeStruct((NC, HID), F32),
        ),
        in_specs=[vmem, vmem],
        out_specs=(vmem, vmem, vmem),
        name='unpack',
    )(sums, count)
    return loss[0, 0], gwh, gwo.T


def solution(mesh):
    row_spec = P(AXIS, None)
    vec_spec = P(AXIS)
    return jax.shard_map(
        device_step, mesh=mesh,
        in_specs=(row_spec, row_spec, P(), P(), vec_spec, vec_spec, P()),
        out_specs=(P(), P(), P()), check_vma=False)
```

```python
import functools

import jax
import jax.numpy as jnp
from jax import lax
from jax.experimental import pallas as pl
from jax.experimental.pallas import tpu as pltpu
from jax.sharding import PartitionSpec as P

AXIS = 'nodes'
MESH = pl.DeviceIdType.MESH
F32, BF16 = jnp.float32, jnp.bfloat16
FIRST = (((0,), (0,)), ((), ()))
LAST = (((1,), (1,)), ((), ()))
NB, BR, FI, HID, NC, CP = 16, 1024, 100, 256, 47, 48
X, Y, Z = 1, 2, 4
DIMS = (X, Y, Z)
NEXT = {X: Y, Y: Z, Z: X}
PREV = {Y: X, Z: Y, X: Z}
XYZ = X + Y + Z
LOSS_LANE = 64

ORDER = [(0, 0), (0, 1)]
for group in ((X, Y, Z), (X + Y, Y + Z, Z + X), (XYZ,)):
    ORDER += [(q, 0) for q in group] + [(q, 1) for q in group]
SLOT = {qc: i for i, qc in enumerate(ORDER)}

AG_COPIES, RS_COPIES = 17, 29
AG_X, AG_Y = 0, AG_COPIES
RS_D2, RS_D1 = 2 * AG_COPIES, 2 * AG_COPIES + RS_COPIES
AR = 2 * AG_COPIES + 2 * RS_COPIES
N_SEM = AR + 60


def peer(me, mask):
    out = me
    for k in range(4):
        if mask >> k & 1:
            out = out + (1 - 2 * (me // (1 << k) % 2)) * (1 << k)
    return out


def kernel(a_hbm, x_hbm, wh_ref, wo_ref, lab_ref, tm_ref,
           sums_ref, count_ref,
           a_v, xg, yg, y1, z1, hid, pos, z2, r2, ra2, rb2, rc2, r1, ra1, rb1, rc1, stage, wop,
           fsrc, frecv, fsum, fall, a_sem, x_sem, send_sem, recv_sem):
    me = lax.axis_index(AXIS)
    devs = {m: peer(me, m) for m in range(16)}

    def rcopy(src, dst, k, mask):
        return pltpu.make_async_remote_copy(
            src_ref=src, dst_ref=dst, send_sem=send_sem.at[k], recv_sem=recv_sem.at[k],
            device_id=(devs[mask],), device_id_type=MESH)

    a_copies = []
    for s, (q, c) in enumerate(ORDER):
        col = pl.multiple_of(devs[2 * q + c] * BR, BR)
        a_copies.append(pltpu.make_async_copy(a_hbm.at[:, pl.ds(col, BR)], a_v.at[s], a_sem.at[s]))
    x_copy = pltpu.make_async_copy(x_hbm, xg.at[0], x_sem)
    x_copy.start()

    barrier = pltpu.get_barrier_semaphore()
    for m in (1, 2, 4, 8):
        pl.semaphore_signal(barrier, inc=1, device_id=(devs[m],), device_id_type=MESH)
    wop[...] = jnp.zeros_like(wop)
    wop[:NC] = wo_ref[...].astype(BF16)
    z2[...] = jnp.zeros_like(z2)
    pl.semaphore_wait(barrier, 4)
    x_copy.wait()

    sent = []

    def start(cp):
        cp.start()
        sent.append(cp)
        return cp

    def gather(base, g, pieces, work, load):
        def core_fwd(q):
            return start(rcopy(g.at[SLOT[q, 0]], g.at[SLOT[q, 1]], base + 9 + q, 1))

        one = {d: start(rcopy(g.at[0], g.at[SLOT[d, 0]], base + i, 2 * d)) for i, d in enumerate(DIMS)}
        half = {0: core_fwd(0)}
        two, three = {}, {}
        load(0)
        work(0, 1)
        half[0].wait_recv()
        work(1, 2)
        for i, d in enumerate(DIMS):
            e = NEXT[d]
            one[e].wait_recv()
            two[d] = start(rcopy(g.at[SLOT[e, 0]], g.at[SLOT[d + e, 0]], base + 3 + i, 2 * d))
        for d in DIMS:
            half[d] = core_fwd(d)
        load(1)
        work(2, 5)
        for d in DIMS:
            half[d].wait_recv()
        work(5, 8)
        for i, d in enumerate(DIMS):
            rows = pl.ds(*pieces[i])
            two[NEXT[d]].wait_recv()
            three[d] = start(rcopy(g.at[SLOT[XYZ - d, 0], rows], g.at[SLOT[XYZ, 0], rows], base + 6 + i, 2 * d))
        for d in DIMS:
            half[XYZ - d] = core_fwd(XYZ - d)
        work(8, 11)
        for d in DIMS:
            three[d].wait_recv()
        half[XYZ] = core_fwd(XYZ)
        for d in DIMS:
            half[XYZ - d].wait_recv()
        work(11, 14)
        half[XYZ].wait_recv()
        work(14, 16)

    wh = wh_ref[...].astype(BF16)

    def load_a(part):
        for s in range(8 * part, 8 * part + 8):
            a_copies[s].start()
        if part == 0:
            z1[...] = jnp.zeros_like(z1)

    def layer_one(lo, hi):
        for s in range(lo, hi):
            a_copies[s].wait()

        def proj(s, ref):
            ref[...] = lax.dot_general(xg[s], wh, FIRST, preferred_element_type=F32).astype(BF16)

        bufs = (hid, y1.at[0], y1.at[1])
        for n, s in enumerate(range(lo, hi)):
            proj(s, bufs[n])
        for n, s in enumerate(range(lo, hi)):
            z1[...] += jnp.dot(a_v[s], bufs[n][...], preferred_element_type=F32)

    gather(AG_X, xg, ((0, 32), (32, 32), (64, 36)), layer_one, load_a)

    hid[...] = jnp.maximum(z1[...], 0.0).astype(BF16)
    tm = tm_ref[...].astype(F32)
    y2t = lax.dot_general(wop[...], hid[...], LAST, preferred_element_type=F32)
    row = lax.broadcasted_iota(jnp.int32, (CP, BR), 0)
    yg[0] = jnp.where(row == NC, tm, y2t).astype(BF16)

    first = [True]

    def layer_two(lo, hi):
        def body(s, carry):
            z2[:, :CP] += lax.dot_general(a_v[s], yg[s], LAST, preferred_element_type=F32)
            return carry

        if 2 <= lo < 8:
            lax.fori_loop(lo, hi, body, 0)
        else:
            for s in range(lo, hi):
                body(s, 0)
        if first[0]:
            first[0] = False
            pos[...] = jnp.where(jnp.transpose(z1[...]) > 0, 1.0, 0.0).astype(BF16)

    gather(AG_Y, yg, ((0, 16), (16, 16), (32, 16)), layer_two, lambda part: None)

    count = jnp.zeros((1, BR), F32)
    for s in range(NB):
        count = count + yg[s, NC:CP, :].astype(F32)
    total = jnp.sum(count, axis=1, keepdims=True)
    zt = jnp.transpose(z2[...])[:CP]
    valid = row < NC
    top = jnp.max(jnp.where(valid, zt, -jnp.inf), axis=0, keepdims=True)
    lse = top + jnp.log(jnp.sum(jnp.where(valid, jnp.exp(zt - top), 0.0), axis=0, keepdims=True))
    hot = row == lab_ref[...]
    picked = jnp.sum(jnp.where(hot, zt, 0.0), axis=0, keepdims=True)
    loss = jnp.sum(tm * (lse - picked), axis=1, keepdims=True)
    grad = (jnp.exp(zt - lse) - hot.astype(F32)) * (tm / total)
    gt = jnp.where(valid, grad, 0.0).astype(BF16)

    def scatter(base, r, ra, rb, rc, pieces, left, stages, early, middle, late):
        def rows(i):
            return pl.ds(*pieces[i])

        pair = {}

        def other(k, q):
            st = stages(k)
            if not early and k >= 2:
                pair[k - 2].wait_send()
                sent[:] = [cp for cp in sent if cp is not pair[k - 2]]
            if early or k == 0:
                st[...] = jnp.dot(left[...], a_v[SLOT[q, 1]], preferred_element_type=F32)
            else:
                def body(h, carry):
                    cols = pl.ds(pl.multiple_of(h * 512, 512), 512)
                    st[:, cols] = jnp.dot(left[...], a_v[SLOT[q, 1], :, cols], preferred_element_type=F32)
                    return carry

                lax.fori_loop(0, 2, body, 0)
            pair[k] = start(rcopy(st, r.at[q], base + k, 1))

        def own(k, q):
            if early:
                mine = jnp.dot(left[...], a_v[SLOT[q, 0]], preferred_element_type=F32)
                pair[k].wait_recv()
                r[q] = r[q] + mine
            else:
                pair[k].wait_recv()

                def body(h, carry):
                    cols = pl.ds(pl.multiple_of(h * 512, 512), 512)
                    r[q, :, cols] = r[q, :, cols] + jnp.dot(left[...], a_v[SLOT[q, 0], :, cols], preferred_element_type=F32)
                    return carry

                lax.fori_loop(0, 2, body, 0)

        def send(q, i, dst, k, d):
            return start(rcopy(r.at[q, rows(i)], dst, k, 2 * d))

        three, two, one = {}, {}, {}
        order = (XYZ,) + tuple(d + NEXT[d] for d in DIMS) + DIMS + (0,)

        def produce(k):
            if k < 7:
                other(k + 1, order[k + 1])
            own(k, order[k])

        other(0, XYZ)
        produce(0)
        for i, d in enumerate(DIMS):
            three[d] = send(XYZ, i, ra.at[rows(i)], base + 8 + i, d)
        for k, d in enumerate(DIMS):
            q = d + NEXT[d]
            produce(1 + k)
            for i, e in enumerate(DIMS):
                if e + q != XYZ:
                    two[d, i] = send(q, i, rb.at[k, rows(i)], base + 11 + 3 * k + i, d)

        def outer():
            for i, e in enumerate(DIMS):
                three[e].wait_recv()
                q = XYZ - e
                r[q, rows(i)] = r[q, rows(i)] + ra[rows(i)]
                d = NEXT[e]
                k = DIMS.index(d)
                two[d, i] = send(q, i, rb.at[k, rows(i)], base + 11 + 3 * k + i, d)

        def inner():
            for j in range(3):
                for n, e in enumerate(DIMS):
                    d = PREV[e]
                    k = DIMS.index(d)
                    last = DIMS.index(XYZ - d - NEXT[d])
                    i = (last + 1 + j) % 3
                    two[d, i].wait_recv()
                    r[e, rows(i)] = r[e, rows(i)] + rb[k, rows(i)]
                    one[e, i] = send(e, i, rc.at[n, rows(i)], base + 20 + 3 * n + i, e)

        if early:
            outer()
        for k, d in enumerate(DIMS):
            produce(4 + k)
        if early:
            inner()
            produce(7)
        else:
            produce(7)
            middle()
            outer()
            inner()
        late()
        for j in range(3):
            for n, e in enumerate(DIMS):
                i = (DIMS.index(XYZ - PREV[e] - e) + 1 + j) % 3
                one[e, i].wait_recv()
                r[0, rows(i)] = r[0, rows(i)] + rc[n, rows(i)]

    def stage_d2(k):
        return stage.at[k // 4, pl.ds(CP * (k % 4), CP)]

    scatter(RS_D2, r2, ra2, rb2, rc2, ((0, 16), (16, 16), (32, 16)), gt, stage_d2, True, None, lambda: None)

    d2t = r2[0].astype(BF16)
    for cp in sent:
        cp.wait_send()
    sent.clear()
    grad_hid = lax.dot_general(wop[...], d2t, FIRST, preferred_element_type=F32)
    pos[...] = jnp.where(pos[...] > 0, grad_hid, 0.0).astype(BF16)

    parts = {}

    def exchange(n, values):
        for i in range(NB):
            fsrc[n, i] = values[16 * i:16 * i + 16]
        k = AR + 30 * n - 1
        parts[n] = [start(rcopy(fsrc.at[n, devs[m]], frecv.at[n, m], k + m, m)) for m in range(1, 16)]

    def share(n):
        acc = fsrc[n, me]
        for m in range(1, 16):
            parts[n][m - 1].wait_recv()
            acc = acc + frecv[n, m]
        fsum[n] = acc
        fall[n, me] = acc
        for m in range(1, 16):
            start(rcopy(fsum.at[n], fall.at[n, me], AR + 30 * n + 14 + m, m))

    def collect(n):
        for m in range(1, 16):
            rcopy(fsum.at[n], fall.at[n, devs[m]], AR + 30 * n + 14 + m, m).wait_recv()

    def middle():
        gwo_t = jnp.dot(d2t, hid[...], preferred_element_type=F32)
        gwo = jnp.transpose(jnp.concatenate([gwo_t, jnp.zeros((128 - CP, HID), F32)], axis=0))
        lane = lax.broadcasted_iota(jnp.int32, (HID, 128), 1)
        exchange(0, jnp.where(lane == LOSS_LANE, loss, gwo))

    def stage_d1(k):
        return stage.at[k % 2]

    scatter(RS_D1, r1, ra1, rb1, rc1, ((0, 88), (88, 88), (176, 80)), pos, stage_d1, False, middle, lambda: share(0))

    d1t = r1[0].astype(BF16)
    gwh_t = lax.dot_general(d1t, xg[0], LAST, preferred_element_type=F32)
    exchange(1, jnp.concatenate([gwh_t, jnp.zeros((HID, 128 - FI), F32)], axis=1))
    share(1)
    collect(0)
    collect(1)
    for n in range(2):
        for i in range(NB):
            sums_ref[n, i] = fall[n, i]
    count_ref[...] = total
    for cp in sent:
        cp.wait_send()


def unpack(sums_ref, count_ref, loss_ref, gwh_ref, gwo_ref):
    gwo, gwh = (jnp.concatenate([sums_ref[n, i] for i in range(NB)], axis=0) for n in range(2))
    gwh_ref[...] = jnp.transpose(gwh)[:FI]
    gwo_ref[...] = jnp.transpose(gwo)[:NC]
    loss_ref[...] = gwo[0:1, LOSS_LANE:LOSS_LANE + 1] / count_ref[...]


def device_step(adj_rows, feat_rows, w_hidden, w_output, labels, train_mask, block_mask):
    del block_mask
    vmem = pl.BlockSpec(memory_space=pltpu.VMEM)
    hbm = pl.BlockSpec(memory_space=pl.ANY)
    sums, count = pl.pallas_call(
        kernel,
        out_shape=(
            jax.ShapeDtypeStruct((2, NB, 16, 128), F32),
            jax.ShapeDtypeStruct((1, 1), F32),
        ),
        in_specs=[hbm, hbm, vmem, vmem, vmem, vmem],
        out_specs=(vmem, vmem),
        scratch_shapes=[
            pltpu.VMEM((NB, BR, BR), BF16),
            pltpu.VMEM((NB, FI, BR), BF16),
            pltpu.VMEM((NB, CP, BR), BF16),
            pltpu.VMEM((2, BR, HID), BF16),
            pltpu.VMEM((BR, HID), F32),
            pltpu.VMEM((BR, HID), BF16),
            pltpu.VMEM((HID, BR), BF16),
            pltpu.VMEM((BR, 128), F32),
            pltpu.VMEM((8, CP, BR), F32),
            pltpu.VMEM((CP, BR), F32),
            pltpu.VMEM((3, CP, BR), F32),
            pltpu.VMEM((3, CP, BR), F32),
            pltpu.VMEM((8, HID, BR), F32),
            pltpu.VMEM((HID, BR), F32),
            pltpu.VMEM((3, HID, BR), F32),
            pltpu.VMEM((3, HID, BR), F32),
            pltpu.VMEM((2, HID, BR), F32),
            pltpu.VMEM((CP, HID), BF16),
            pltpu.VMEM((2, NB, 16, 128), F32),
            pltpu.VMEM((2, NB, 16, 128), F32),
            pltpu.VMEM((2, 16, 128), F32),
            pltpu.VMEM((2, NB, 16, 128), F32),
            pltpu.SemaphoreType.DMA((NB,)),
            pltpu.SemaphoreType.DMA,
            pltpu.SemaphoreType.DMA((N_SEM,)),
            pltpu.SemaphoreType.DMA((N_SEM,)),
        ],
        compiler_params=pltpu.CompilerParams(
            collective_id=0, has_side_effects=True, vmem_limit_bytes=67_043_328),
        name='gcn_step',
    )(adj_rows, feat_rows.T, w_hidden, w_output.T, labels.reshape(1, -1), train_mask.reshape(1, -1))
    loss, gwh, gwo = pl.pallas_call(
        unpack,
        out_shape=(
            jax.ShapeDtypeStruct((1, 1), F32),
            jax.ShapeDtypeStruct((FI, HID), F32),
            jax.ShapeDtypeStruct((NC, HID), F32),
        ),
        in_specs=[vmem, vmem],
        out_specs=(vmem, vmem, vmem),
        name='unpack',
    )(sums, count)
    return loss[0, 0], gwh, gwo.T


def solution(mesh):
    row_spec = P(AXIS, None)
    vec_spec = P(AXIS)
    return jax.shard_map(
        device_step, mesh=mesh,
        in_specs=(row_spec, row_spec, P(), P(), vec_spec, vec_spec, P()),
        out_specs=(P(), P(), P()), check_vma=False)
```

```python
import functools

import jax
import jax.numpy as jnp
from jax import lax
from jax.experimental import pallas as pl
from jax.experimental.pallas import tpu as pltpu
from jax.sharding import PartitionSpec as P

AXIS = 'nodes'
MESH = pl.DeviceIdType.MESH
F32, BF16 = jnp.float32, jnp.bfloat16
FIRST = (((0,), (0,)), ((), ()))
LAST = (((1,), (1,)), ((), ()))
NB, BR, FI, HID, NC, CP = 16, 1024, 100, 256, 47, 48
X, Y, Z = 1, 2, 4
DIMS = (X, Y, Z)
NEXT = {X: Y, Y: Z, Z: X}
PREV = {Y: X, Z: Y, X: Z}
XYZ = X + Y + Z
LOSS_LANE = 64
HID_PIECES = ((0, 88), (88, 88), (176, 80))
TURN = {X: (0, 1, 2), Y: (1, 0, 2), Z: (0, 1, 2)}

ORDER = [(0, 0), (0, 1)]
for group in ((X, Y, Z), (X + Y, Y + Z, Z + X), (XYZ,)):
    ORDER += [(q, 0) for q in group] + [(q, 1) for q in group]
SLOT = {qc: i for i, qc in enumerate(ORDER)}

AG_COPIES, RS_COPIES = 17, 29
AG_X, AG_Y = 0, AG_COPIES
RS_D2, RS_D1 = 2 * AG_COPIES, 2 * AG_COPIES + RS_COPIES
AR = 2 * AG_COPIES + 2 * RS_COPIES
N_SEM = AR + 120


def peer(me, mask):
    out = me
    for k in range(4):
        if mask >> k & 1:
            out = out + (1 - 2 * (me // (1 << k) % 2)) * (1 << k)
    return out


def kernel(a_hbm, x_hbm, wh_ref, wo_ref, lab_ref, tm_ref,
           osums_ref, hsums_ref, count_ref,
           a_v, xg, yg, y1, z1, hid, pos, z2, r2, ra2, rb2, rc2, r1, ra1, rb1, rc1, stage, wop,
           osrc, orecv, osum, oall, hsrc, hrecv, hsum, hall, a_sem, x_sem, send_sem, recv_sem):
    me = lax.axis_index(AXIS)
    devs = {m: peer(me, m) for m in range(16)}

    def rcopy(src, dst, k, mask):
        return pltpu.make_async_remote_copy(
            src_ref=src, dst_ref=dst, send_sem=send_sem.at[k], recv_sem=recv_sem.at[k],
            device_id=(devs[mask],), device_id_type=MESH)

    a_copies = []
    for s, (q, c) in enumerate(ORDER):
        col = pl.multiple_of(devs[2 * q + c] * BR, BR)
        a_copies.append(pltpu.make_async_copy(a_hbm.at[:, pl.ds(col, BR)], a_v.at[s], a_sem.at[s]))
    x_copy = pltpu.make_async_copy(x_hbm, xg.at[0], x_sem)
    x_copy.start()

    barrier = pltpu.get_barrier_semaphore()
    for m in (1, 2, 4, 8):
        pl.semaphore_signal(barrier, inc=1, device_id=(devs[m],), device_id_type=MESH)
    wop[...] = jnp.zeros_like(wop)
    wop[:NC] = wo_ref[...].astype(BF16)
    z2[...] = jnp.zeros_like(z2)
    pl.semaphore_wait(barrier, 4)
    x_copy.wait()

    sent = []

    def start(cp):
        cp.start()
        sent.append(cp)
        return cp

    def gather(base, g, pieces, work, load):
        def core_fwd(q):
            return start(rcopy(g.at[SLOT[q, 0]], g.at[SLOT[q, 1]], base + 9 + q, 1))

        one = {d: start(rcopy(g.at[0], g.at[SLOT[d, 0]], base + i, 2 * d)) for i, d in enumerate(DIMS)}
        half = {0: core_fwd(0)}
        two, three = {}, {}
        load(0)
        work(0, 1)
        half[0].wait_recv()
        work(1, 2)
        for i, d in enumerate(DIMS):
            e = NEXT[d]
            one[e].wait_recv()
            two[d] = start(rcopy(g.at[SLOT[e, 0]], g.at[SLOT[d + e, 0]], base + 3 + i, 2 * d))
        for d in DIMS:
            half[d] = core_fwd(d)
        load(1)
        work(2, 5)
        for d in DIMS:
            half[d].wait_recv()
        work(5, 8)
        for i, d in enumerate(DIMS):
            rows = pl.ds(*pieces[i])
            two[NEXT[d]].wait_recv()
            three[d] = start(rcopy(g.at[SLOT[XYZ - d, 0], rows], g.at[SLOT[XYZ, 0], rows], base + 6 + i, 2 * d))
        for d in DIMS:
            half[XYZ - d] = core_fwd(XYZ - d)
        work(8, 11)
        for d in DIMS:
            three[d].wait_recv()
        half[XYZ] = core_fwd(XYZ)
        for d in DIMS:
            half[XYZ - d].wait_recv()
        work(11, 14)
        half[XYZ].wait_recv()
        work(14, 16)

    wh = wh_ref[...].astype(BF16)

    def load_a(part):
        for s in range(8 * part, 8 * part + 8):
            a_copies[s].start()
        if part == 0:
            z1[...] = jnp.zeros_like(z1)
            hsrc[...] = jnp.zeros_like(hsrc)

    def layer_one(lo, hi):
        for s in range(lo, hi):
            a_copies[s].wait()

        def proj(s, ref):
            ref[...] = lax.dot_general(xg[s], wh, FIRST, preferred_element_type=F32).astype(BF16)

        bufs = (hid, y1.at[0], y1.at[1])
        for n, s in enumerate(range(lo, hi)):
            proj(s, bufs[n])
        for n, s in enumerate(range(lo, hi)):
            z1[...] += jnp.dot(a_v[s], bufs[n][...], preferred_element_type=F32)

    gather(AG_X, xg, ((0, 32), (32, 32), (64, 36)), layer_one, load_a)

    hid[...] = jnp.maximum(z1[...], 0.0).astype(BF16)
    tm = tm_ref[...].astype(F32)
    y2t = lax.dot_general(wop[...], hid[...], LAST, preferred_element_type=F32)
    row = lax.broadcasted_iota(jnp.int32, (CP, BR), 0)
    yg[0] = jnp.where(row == NC, tm, y2t).astype(BF16)

    first = [True]

    def layer_two(lo, hi):
        def body(s, carry):
            z2[:, :CP] += lax.dot_general(a_v[s], yg[s], LAST, preferred_element_type=F32)
            return carry

        if 2 <= lo < 8:
            lax.fori_loop(lo, hi, body, 0)
        else:
            for s in range(lo, hi):
                body(s, 0)
        if first[0]:
            first[0] = False
            pos[...] = jnp.where(jnp.transpose(z1[...]) > 0, 1.0, 0.0).astype(BF16)

    gather(AG_Y, yg, ((0, 16), (16, 16), (32, 16)), layer_two, lambda part: None)

    count = jnp.zeros((1, BR), F32)
    for s in range(NB):
        count = count + yg[s, NC:CP, :].astype(F32)
    total = jnp.sum(count, axis=1, keepdims=True)
    zt = jnp.transpose(z2[...])[:CP]
    valid = row < NC
    top = jnp.max(jnp.where(valid, zt, -jnp.inf), axis=0, keepdims=True)
    lse = top + jnp.log(jnp.sum(jnp.where(valid, jnp.exp(zt - top), 0.0), axis=0, keepdims=True))
    hot = row == lab_ref[...]
    picked = jnp.sum(jnp.where(hot, zt, 0.0), axis=0, keepdims=True)
    loss = jnp.sum(tm * (lse - picked), axis=1, keepdims=True)
    grad = (jnp.exp(zt - lse) - hot.astype(F32)) * (tm / total)
    gt = jnp.where(valid, grad, 0.0).astype(BF16)

    def scatter(base, r, ra, rb, rc, pieces, left, stages, early, middle, late, final):
        def rows(i):
            return pl.ds(*pieces[i])

        pair = {}

        def other(k, q):
            st = stages(k)
            if not early and k >= 2:
                pair[k - 2].wait_send()
                sent[:] = [cp for cp in sent if cp is not pair[k - 2]]
            if early or k == 0:
                st[...] = jnp.dot(left[...], a_v[SLOT[q, 1]], preferred_element_type=F32)
            else:
                def body(h, carry):
                    cols = pl.ds(pl.multiple_of(h * 512, 512), 512)
                    st[:, cols] = jnp.dot(left[...], a_v[SLOT[q, 1], :, cols], preferred_element_type=F32)
                    return carry

                lax.fori_loop(0, 2, body, 0)
            pair[k] = start(rcopy(st, r.at[q], base + k, 1))

        def own(k, q):
            if early:
                mine = jnp.dot(left[...], a_v[SLOT[q, 0]], preferred_element_type=F32)
                pair[k].wait_recv()
                r[q] = r[q] + mine
            else:
                pair[k].wait_recv()

                def body(h, carry):
                    cols = pl.ds(pl.multiple_of(h * 512, 512), 512)
                    r[q, :, cols] = r[q, :, cols] + jnp.dot(left[...], a_v[SLOT[q, 0], :, cols], preferred_element_type=F32)
                    return carry

                lax.fori_loop(0, 2, body, 0)

        def send(q, i, dst, k, d):
            return start(rcopy(r.at[q, rows(i)], dst, k, 2 * d))

        three, two, one = {}, {}, {}
        order = (XYZ,) + tuple(d + NEXT[d] for d in DIMS) + DIMS + (0,)

        def produce(k):
            if k < 7:
                other(k + 1, order[k + 1])
            own(k, order[k])

        other(0, XYZ)
        produce(0)
        for i, d in enumerate(DIMS):
            three[d] = send(XYZ, i, ra.at[rows(i)], base + 8 + i, d)
        for k, d in enumerate(DIMS):
            q = d + NEXT[d]
            produce(1 + k)
            for i in TURN[d]:
                if DIMS[i] + q == XYZ:
                    break
                two[d, i] = send(q, i, rb.at[k, rows(i)], base + 11 + 3 * k + i, d)

        def outer():
            for i, e in enumerate(DIMS):
                three[e].wait_recv()
                q = XYZ - e
                r[q, rows(i)] = r[q, rows(i)] + ra[rows(i)]
                d = NEXT[e]
                k = DIMS.index(d)
                for n in TURN[d][TURN[d].index(i):]:
                    two[d, n] = send(q, n, rb.at[k, rows(n)], base + 11 + 3 * k + n, d)

        def inner():
            for j in range(3):
                for n, e in enumerate(DIMS):
                    d = PREV[e]
                    k = DIMS.index(d)
                    i = TURN[d][j]
                    two[d, i].wait_recv()
                    r[e, rows(i)] = r[e, rows(i)] + rb[k, rows(i)]
                    one[e, i] = send(e, i, rc.at[n, rows(i)], base + 20 + 3 * n + i, e)

        if early:
            outer()
        for k, d in enumerate(DIMS):
            produce(4 + k)
            if k == 1 and not early:
                outer()
        if early:
            inner()
            produce(7)
        else:
            produce(7)
            middle()
            inner()
        late()
        for j in range(3):
            for n, e in enumerate(DIMS):
                i = TURN[PREV[e]][j]
                one[e, i].wait_recv()
                r[0, rows(i)] = r[0, rows(i)] + rc[n, rows(i)]
            for i in ((), (0, 1), (2,))[j]:
                final(i)

    def stage_d2(k):
        return stage.at[k // 4, pl.ds(CP * (k % 4), CP)]

    scatter(RS_D2, r2, ra2, rb2, rc2, ((0, 16), (16, 16), (32, 16)), gt, stage_d2, True, None, lambda: None, lambda i: None)

    d2t = r2[0].astype(BF16)
    for cp in sent:
        cp.wait_send()
    sent.clear()
    grad_hid = lax.dot_general(wop[...], d2t, FIRST, preferred_element_type=F32)
    pos[...] = jnp.where(pos[...] > 0, grad_hid, 0.0).astype(BF16)

    parts = {}
    bufs = [(osrc, orecv, osum, oall)] + [(hsrc.at[i], hrecv.at[i], hsum.at[i], hall.at[i]) for i in range(3)]

    def exchange(n, values):
        src, recv, _, _ = bufs[n]
        per = -(-values.shape[0] // NB)
        for i in range(0, NB):
            rows = values[per * i:per * i + per]
            if rows.shape[0]:
                src[i, 0:rows.shape[0], 0:rows.shape[1]] = rows
        k = AR + 30 * n - 1
        parts[n] = [start(rcopy(src.at[devs[m]], recv.at[m], k + m, m)) for m in range(1, 16)]

    def share(n):
        src, recv, total_n, out = bufs[n]
        acc = src[me]
        for m in range(1, 16):
            parts[n][m - 1].wait_recv()
            acc = acc + recv[m]
        total_n[...] = acc
        out[me] = acc
        for m in range(1, 16):
            start(rcopy(total_n, out.at[me], AR + 30 * n + 14 + m, m))

    def collect(n):
        _, _, total_n, out = bufs[n]
        for m in range(1, 16):
            rcopy(total_n, out.at[devs[m]], AR + 30 * n + 14 + m, m).wait_recv()

    def hidden_grad(i):
        d1t = r1[0, pl.ds(*HID_PIECES[i])].astype(BF16)
        exchange(1 + i, lax.dot_general(d1t, xg[0], LAST, preferred_element_type=F32))

    def middle():
        gwo_t = jnp.dot(d2t, hid[...], preferred_element_type=F32)
        gwo = jnp.transpose(jnp.concatenate([gwo_t, jnp.zeros((128 - CP, HID), F32)], axis=0))
        lane = lax.broadcasted_iota(jnp.int32, (HID, 128), 1)
        exchange(0, jnp.where(lane == LOSS_LANE, loss, gwo))

    def stage_d1(k):
        return stage.at[k % 2]

    scatter(RS_D1, r1, ra1, rb1, rc1, HID_PIECES, pos, stage_d1, False, middle, lambda: share(0), hidden_grad)

    for n in range(1, 4):
        share(n)
    for n in range(4):
        collect(n)
    osums_ref[...] = oall[...]
    hsums_ref[...] = hall[...]
    count_ref[...] = total
    for cp in sent:
        cp.wait_send()


def unpack(osums_ref, hsums_ref, count_ref, loss_ref, gwh_ref, gwo_ref, rows_ref):
    gwo = jnp.concatenate([osums_ref[i] for i in range(NB)], axis=0)
    for p, (lo, size) in enumerate(HID_PIECES):
        per = -(-size // NB)
        for i in range(NB):
            rows_ref[lo + per * i:lo + per * i + per] = hsums_ref[p, i, 0:per]
    gwh = rows_ref[0:HID]
    gwh_ref[...] = jnp.transpose(gwh)[:FI]
    gwo_ref[...] = jnp.transpose(gwo)[:NC]
    loss_ref[...] = gwo[0:1, LOSS_LANE:LOSS_LANE + 1] / count_ref[...]


def device_step(adj_rows, feat_rows, w_hidden, w_output, labels, train_mask, block_mask):
    del block_mask
    vmem = pl.BlockSpec(memory_space=pltpu.VMEM)
    hbm = pl.BlockSpec(memory_space=pl.ANY)
    osums, hsums, count = pl.pallas_call(
        kernel,
        out_shape=(
            jax.ShapeDtypeStruct((NB, 16, 128), F32),
            jax.ShapeDtypeStruct((3, NB, 8, 128), F32),
            jax.ShapeDtypeStruct((1, 1), F32),
        ),
        in_specs=[hbm, hbm, vmem, vmem, vmem, vmem],
        out_specs=(vmem, vmem, vmem),
        scratch_shapes=[
            pltpu.VMEM((NB, BR, BR), BF16),
            pltpu.VMEM((NB, FI, BR), BF16),
            pltpu.VMEM((NB, CP, BR), BF16),
            pltpu.VMEM((2, BR, HID), BF16),
            pltpu.VMEM((BR, HID), F32),
            pltpu.VMEM((BR, HID), BF16),
            pltpu.VMEM((HID, BR), BF16),
            pltpu.VMEM((BR, 128), F32),
            pltpu.VMEM((8, CP, BR), F32),
            pltpu.VMEM((CP, BR), F32),
            pltpu.VMEM((3, CP, BR), F32),
            pltpu.VMEM((3, CP, BR), F32),
            pltpu.VMEM((8, HID, BR), F32),
            pltpu.VMEM((HID, BR), F32),
            pltpu.VMEM((3, HID, BR), F32),
            pltpu.VMEM((3, HID, BR), F32),
            pltpu.VMEM((2, HID, BR), F32),
            pltpu.VMEM((CP, HID), BF16),
            pltpu.VMEM((NB, 16, 128), F32),
            pltpu.VMEM((NB, 16, 128), F32),
            pltpu.VMEM((16, 128), F32),
            pltpu.VMEM((NB, 16, 128), F32),
            pltpu.VMEM((3, NB, 8, 128), F32),
            pltpu.VMEM((3, NB, 8, 128), F32),
            pltpu.VMEM((3, 8, 128), F32),
            pltpu.VMEM((3, NB, 8, 128), F32),
            pltpu.SemaphoreType.DMA((NB,)),
            pltpu.SemaphoreType.DMA,
            pltpu.SemaphoreType.DMA((N_SEM,)),
            pltpu.SemaphoreType.DMA((N_SEM,)),
        ],
        compiler_params=pltpu.CompilerParams(
            collective_id=0, has_side_effects=True, vmem_limit_bytes=67_043_328),
        name='gcn_step',
    )(adj_rows, feat_rows.T, w_hidden, w_output.T, labels.reshape(1, -1), train_mask.reshape(1, -1))
    loss, gwh, gwo = pl.pallas_call(
        unpack,
        out_shape=(
            jax.ShapeDtypeStruct((1, 1), F32),
            jax.ShapeDtypeStruct((FI, HID), F32),
            jax.ShapeDtypeStruct((NC, HID), F32),
        ),
        in_specs=[vmem, vmem, vmem],
        out_specs=(vmem, vmem, vmem),
        scratch_shapes=[pltpu.VMEM((HID + 16, 128), F32)],
        name='unpack',
    )(osums, hsums, count)
    return loss[0, 0], gwh, gwo.T


def solution(mesh):
    row_spec = P(AXIS, None)
    vec_spec = P(AXIS)
    return jax.shard_map(
        device_step, mesh=mesh,
        in_specs=(row_spec, row_spec, P(), P(), vec_spec, vec_spec, P()),
        out_specs=(P(), P(), P()), check_vma=False)
```

```python
import functools

import jax
import jax.numpy as jnp
from jax import lax
from jax.experimental import pallas as pl
from jax.experimental.pallas import tpu as pltpu
from jax.sharding import PartitionSpec as P

AXIS = 'nodes'
MESH = pl.DeviceIdType.MESH
F32, BF16 = jnp.float32, jnp.bfloat16
FIRST = (((0,), (0,)), ((), ()))
LAST = (((1,), (1,)), ((), ()))
NB, BR, FI, HID, NC, CP = 16, 1024, 100, 256, 47, 48
X, Y, Z = 1, 2, 4
DIMS = (X, Y, Z)
NEXT = {X: Y, Y: Z, Z: X}
PREV = {Y: X, Z: Y, X: Z}
XYZ = X + Y + Z
LOSS_LANE = 64

PLACES = (0, X, Y, Z, X + Y, Y + Z, Z + X, XYZ)
PLACE = {q: j for j, q in enumerate(PLACES)}
ORDER = [(q, c) for q in PLACES for c in (0, 1)]
SLOT = {qc: i for i, qc in enumerate(ORDER)}

AG_COPIES, RS_COPIES = 17, 31
AG_X, AG_Y = 0, AG_COPIES
RS_D2, RS_D1 = 2 * AG_COPIES, 2 * AG_COPIES + RS_COPIES
AR = 2 * AG_COPIES + 2 * RS_COPIES
N_SEM = AR + 60


def peer(me, mask):
    out = me
    for k in range(4):
        if mask >> k & 1:
            out = out + (1 - 2 * (me // (1 << k) % 2)) * (1 << k)
    return out


def kernel(a_hbm, x_hbm, wh_ref, wo_ref, lab_ref, tm_ref,
           sums_ref, count_ref,
           a_v, xg, yg, y1, z1, hid, pos, z2, r2, ra2, rb2, rc2, r1, ra1, rb1, rc1, stage, wop,
           fsrc, frecv, fsum, fall, a_sem, x_sem, send_sem, recv_sem):
    me = lax.axis_index(AXIS)
    devs = {m: peer(me, m) for m in range(16)}

    def rcopy(src, dst, k, mask):
        return pltpu.make_async_remote_copy(
            src_ref=src, dst_ref=dst, send_sem=send_sem.at[k], recv_sem=recv_sem.at[k],
            device_id=(devs[mask],), device_id_type=MESH)

    a_copies = []
    for s, (q, c) in enumerate(ORDER):
        col = pl.multiple_of(devs[2 * q + c] * BR, BR)
        a_copies.append(pltpu.make_async_copy(a_hbm.at[:, pl.ds(col, BR)], a_v.at[s], a_sem.at[s]))
    x_copy = pltpu.make_async_copy(x_hbm, xg.at[0], x_sem)
    x_copy.start()

    barrier = pltpu.get_barrier_semaphore()
    for m in (1, 2, 4, 8):
        pl.semaphore_signal(barrier, inc=1, device_id=(devs[m],), device_id_type=MESH)
    wop[...] = jnp.zeros_like(wop)
    wop[:NC] = wo_ref[...].astype(BF16)
    z2[...] = jnp.zeros_like(z2)
    pl.semaphore_wait(barrier, 4)
    x_copy.wait()

    sent = []

    def start(cp):
        cp.start()
        sent.append(cp)
        return cp

    def gather(base, g, pieces, work, load):
        one, two, three = {}, {}, {}
        half = {q: rcopy(g.at[SLOT[q, 0]], g.at[SLOT[q, 1]], base + 9 + q, 1) for q in PLACES}
        for i, d in enumerate(DIMS):
            e, rows = NEXT[d], pl.ds(*pieces[i])
            one[d] = rcopy(g.at[0], g.at[SLOT[d, 0]], base + i, 2 * d)
            two[d] = rcopy(g.at[SLOT[e, 0]], g.at[SLOT[d + e, 0]], base + 3 + i, 2 * d)
            three[d] = rcopy(g.at[SLOT[XYZ - d, 0], rows], g.at[SLOT[XYZ, 0], rows], base + 6 + i, 2 * d)
        for d in DIMS:
            start(one[d])
        start(half[0])
        load(0)

        def second():
            for d in DIMS:
                one[NEXT[d]].wait_recv()
                start(two[d])
            for d in DIMS:
                start(half[d])
            load(1)

        def third():
            for d in DIMS:
                two[NEXT[d]].wait_recv()
                start(three[d])
            for d in DIMS:
                start(half[XYZ - d])
            half[Z].wait_recv()

        def fourth():
            for d in DIMS:
                three[d].wait_recv()
            start(half[XYZ])
            half[Y + Z].wait_recv()

        events = {2: second, 7: third, 11: fourth}
        for q in PLACES:
            events.setdefault(SLOT[q, 1], half[q].wait_recv)

        def step(n, carry):
            for at, event in events.items():
                pl.when(n == at)(event)
            work(n)
            return carry

        lax.fori_loop(0, NB, step, 0)

    def gather_straight(base, g, pieces, work, load):
        def core_fwd(q):
            return start(rcopy(g.at[SLOT[q, 0]], g.at[SLOT[q, 1]], base + 9 + q, 1))

        one = {d: start(rcopy(g.at[0], g.at[SLOT[d, 0]], base + i, 2 * d)) for i, d in enumerate(DIMS)}
        half = {0: core_fwd(0)}
        two, three = {}, {}
        load(0)
        work([0])
        half[0].wait_recv()
        work([1])
        for i, d in enumerate(DIMS):
            e = NEXT[d]
            one[e].wait_recv()
            two[d] = start(rcopy(g.at[SLOT[e, 0]], g.at[SLOT[d + e, 0]], base + 3 + i, 2 * d))
        for d in DIMS:
            half[d] = core_fwd(d)
        load(1)
        work([2, 4, 6])
        for d in DIMS:
            half[d].wait_recv()
        work([3, 5])
        for i, d in enumerate(DIMS):
            rows = pl.ds(*pieces[i])
            two[NEXT[d]].wait_recv()
            three[d] = start(rcopy(g.at[SLOT[XYZ - d, 0], rows], g.at[SLOT[XYZ, 0], rows], base + 6 + i, 2 * d))
        for d in DIMS:
            half[XYZ - d] = core_fwd(XYZ - d)
        work([7, 8, 10])
        work([12])
        for d in DIMS:
            three[d].wait_recv()
        half[XYZ] = core_fwd(XYZ)
        for d in DIMS:
            half[XYZ - d].wait_recv()
        work([9, 11, 13])
        half[XYZ].wait_recv()
        work([14, 15])

    wh = wh_ref[...].astype(BF16)

    def load_a(part):
        for s in range(8 * part, 8 * part + 8):
            a_copies[s].start()
        if part == 0:
            z1[...] = jnp.zeros_like(z1)

    def layer_one(slots):
        bufs = (hid, y1.at[0], y1.at[1])
        for s in slots:
            a_copies[s].wait()
        for n, s in enumerate(slots):
            bufs[n][...] = lax.dot_general(xg[s], wh, FIRST, preferred_element_type=F32).astype(BF16)
        for n, s in enumerate(slots):
            z1[...] += jnp.dot(a_v[s], bufs[n][...], preferred_element_type=F32)

    gather_straight(AG_X, xg, ((0, 32), (32, 32), (64, 36)), layer_one, load_a)

    hid[...] = jnp.maximum(z1[...], 0.0).astype(BF16)
    tm = tm_ref[...].astype(F32)
    y2t = lax.dot_general(wop[...], hid[...], LAST, preferred_element_type=F32)
    row = lax.broadcasted_iota(jnp.int32, (CP, BR), 0)
    yg[0] = jnp.where(row == NC, tm, y2t).astype(BF16)

    def layer_two(n):
        z2[:, :CP] += lax.dot_general(a_v[n], yg[n], LAST, preferred_element_type=F32)

    def keep_sign(part):
        if part == 0:
            pos[...] = jnp.where(jnp.transpose(z1[...]) > 0, 1.0, 0.0).astype(BF16)

    gather(AG_Y, yg, ((0, 16), (16, 16), (32, 16)), layer_two, keep_sign)

    count = jnp.zeros((1, BR), F32)
    for s in range(NB):
        count = count + yg[s, NC:CP, :].astype(F32)
    total = jnp.sum(count, axis=1, keepdims=True)
    zt = jnp.transpose(z2[...])[:CP]
    valid = row < NC
    top = jnp.max(jnp.where(valid, zt, -jnp.inf), axis=0, keepdims=True)
    lse = top + jnp.log(jnp.sum(jnp.where(valid, jnp.exp(zt - top), 0.0), axis=0, keepdims=True))
    hot = row == lab_ref[...]
    picked = jnp.sum(jnp.where(hot, zt, 0.0), axis=0, keepdims=True)
    loss = jnp.sum(tm * (lse - picked), axis=1, keepdims=True)
    grad = (jnp.exp(zt - lse) - hot.astype(F32)) * (tm / total)
    gt = jnp.where(valid, grad, 0.0).astype(BF16)

    def scatter(base, r, ra, rb, rc, pieces, left, early, middle, late):
        def rows(i):
            return pl.ds(*pieces[i])

        def pair(k):
            return rcopy(stage.at[k % 2, pl.ds(0, left.shape[0])], r.at[7 - k], base + k, 1)

        def other(k):
            pl.when(k >= (2 if early else 3))(lambda: pair(k - 2).wait_send())
            stage[k % 2, 0:left.shape[0]] = jnp.dot(left[...], a_v[15 - 2 * k], preferred_element_type=F32)
            pair(k).start()

        def own(k):
            if early:
                mine = jnp.dot(left[...], a_v[14 - 2 * k], preferred_element_type=F32)
                pair(k).wait_recv()
                r[7 - k] = r[7 - k] + mine
            else:
                pair(k).wait_recv()
                r[7 - k] = r[7 - k] + jnp.dot(left[...], a_v[14 - 2 * k], preferred_element_type=F32)

        def send(q, i, dst, k, d):
            return rcopy(r.at[PLACE[q], rows(i)], dst, k, 2 * d)

        three, two, one = {}, {}, {}
        for k, d in enumerate(DIMS):
            q = d + NEXT[d]
            three[d] = send(XYZ, k, ra.at[rows(k)], base + 8 + k, d)
            for i in range(3):
                two[d, i] = send(q, i, rb.at[k, rows(i)], base + 11 + 3 * k + i, d)
                one[d, i] = send(d, i, rc.at[k, rows(i)], base + 20 + 3 * k + i, d)

        def corner():
            for d in DIMS:
                start(three[d])

        def edge(d):
            for i, e in enumerate(DIMS):
                if e + d + NEXT[d] != XYZ:
                    start(two[d, i])

        def outer():
            for i, e in enumerate(DIMS):
                three[e].wait_recv()
                j = PLACE[XYZ - e]
                r[j, rows(i)] = r[j, rows(i)] + ra[rows(i)]
                start(two[NEXT[e], i])

        def inner():
            for j in range(3):
                for e in DIMS:
                    d = PREV[e]
                    k = DIMS.index(d)
                    i = (DIMS.index(XYZ - d - e) + 1 + j) % 3
                    two[d, i].wait_recv()
                    r[PLACE[e], rows(i)] = r[PLACE[e], rows(i)] + rb[k, rows(i)]
                    start(one[e, i])

        def edges():
            edge(X)
            if early:
                outer()

        events = {1: corner, 2: lambda: edge(Z), 3: lambda: edge(Y), 4: edges}
        if early:
            events[7] = inner

        def step(k, carry):
            pl.when(k < 8)(lambda: other(k))
            pl.when(k >= 1)(lambda: own(k - 1))
            for at, event in events.items():
                pl.when(k == at)(event)
            return carry

        if early:
            lax.fori_loop(0, 9, step, 0)
        else:
            stage[0] = jnp.dot(left[...], a_v[15], preferred_element_type=F32)
            thirds = [
                rcopy(stage.at[0, rows(i)], r.at[7, rows(i)], base + (0, 29, 30)[i], 1) for i in range(3)]
            for cp in thirds:
                cp.start()
            stage[1] = jnp.dot(left[...], a_v[14], preferred_element_type=F32)
            for i, d in enumerate(DIMS):
                thirds[i].wait_recv()
                r[7, rows(i)] = r[7, rows(i)] + stage[1, rows(i)]
                start(three[d])
            stage[1] = jnp.dot(left[...], a_v[13], preferred_element_type=F32)
            pair(1).start()
            for cp in thirds:
                cp.wait_send()
            events.pop(1)
            lax.fori_loop(2, 9, step, 0)
        for k in (6, 7):
            pair(k).wait_send()
        if not early:
            middle()
            outer()
            inner()
        late()
        for j in range(3):
            for n, e in enumerate(DIMS):
                i = (DIMS.index(XYZ - PREV[e] - e) + 1 + j) % 3
                one[e, i].wait_recv()
                r[0, rows(i)] = r[0, rows(i)] + rc[n, rows(i)]

    scatter(RS_D2, r2, ra2, rb2, rc2, ((0, 16), (16, 16), (32, 16)), gt, True, None, lambda: None)

    d2t = r2[0].astype(BF16)
    for cp in sent:
        cp.wait_send()
    sent.clear()
    grad_hid = lax.dot_general(wop[...], d2t, FIRST, preferred_element_type=F32)
    pos[...] = jnp.where(pos[...] > 0, grad_hid, 0.0).astype(BF16)

    parts = {}

    def exchange(n, values):
        for i in range(NB):
            fsrc[n, i] = values[16 * i:16 * i + 16]
        k = AR + 30 * n - 1
        parts[n] = [start(rcopy(fsrc.at[n, devs[m]], frecv.at[n, m], k + m, m)) for m in range(1, 16)]

    def share(n):
        acc = fsrc[n, me]
        for m in range(1, 16):
            parts[n][m - 1].wait_recv()
            acc = acc + frecv[n, m]
        fsum[n] = acc
        fall[n, me] = acc
        for m in range(1, 16):
            start(rcopy(fsum.at[n], fall.at[n, me], AR + 30 * n + 14 + m, m))

    def collect(n):
        for m in range(1, 16):
            rcopy(fsum.at[n], fall.at[n, devs[m]], AR + 30 * n + 14 + m, m).wait_recv()

    def middle():
        gwo_t = jnp.dot(d2t, hid[...], preferred_element_type=F32)
        gwo = jnp.transpose(jnp.concatenate([gwo_t, jnp.zeros((128 - CP, HID), F32)], axis=0))
        lane = lax.broadcasted_iota(jnp.int32, (HID, 128), 1)
        exchange(0, jnp.where(lane == LOSS_LANE, loss, gwo))

    scatter(RS_D1, r1, ra1, rb1, rc1, ((0, 88), (88, 88), (176, 80)), pos, False, middle, lambda: share(0))

    d1t = r1[0].astype(BF16)
    gwh_t = lax.dot_general(d1t, xg[0], LAST, preferred_element_type=F32)
    exchange(1, jnp.concatenate([gwh_t, jnp.zeros((HID, 128 - FI), F32)], axis=1))
    share(1)
    collect(0)
    collect(1)
    for n in range(2):
        for i in range(NB):
            sums_ref[n, i] = fall[n, i]
    count_ref[...] = total
    for cp in sent:
        cp.wait_send()


def unpack(sums_ref, count_ref, loss_ref, gwh_ref, gwo_ref):
    gwo, gwh = (jnp.concatenate([sums_ref[n, i] for i in range(NB)], axis=0) for n in range(2))
    gwh_ref[...] = jnp.transpose(gwh)[:FI]
    gwo_ref[...] = jnp.transpose(gwo)[:NC]
    loss_ref[...] = gwo[0:1, LOSS_LANE:LOSS_LANE + 1] / count_ref[...]


def device_step(adj_rows, feat_rows, w_hidden, w_output, labels, train_mask, block_mask):
    del block_mask
    vmem = pl.BlockSpec(memory_space=pltpu.VMEM)
    hbm = pl.BlockSpec(memory_space=pl.ANY)
    sums, count = pl.pallas_call(
        kernel,
        out_shape=(
            jax.ShapeDtypeStruct((2, NB, 16, 128), F32),
            jax.ShapeDtypeStruct((1, 1), F32),
        ),
        in_specs=[hbm, hbm, vmem, vmem, vmem, vmem],
        out_specs=(vmem, vmem),
        scratch_shapes=[
            pltpu.VMEM((NB, BR, BR), BF16),
            pltpu.VMEM((NB, FI, BR), BF16),
            pltpu.VMEM((NB, CP, BR), BF16),
            pltpu.VMEM((2, BR, HID), BF16),
            pltpu.VMEM((BR, HID), F32),
            pltpu.VMEM((BR, HID), BF16),
            pltpu.VMEM((HID, BR), BF16),
            pltpu.VMEM((BR, 128), F32),
            pltpu.VMEM((8, CP, BR), F32),
            pltpu.VMEM((CP, BR), F32),
            pltpu.VMEM((3, CP, BR), F32),
            pltpu.VMEM((3, CP, BR), F32),
            pltpu.VMEM((8, HID, BR), F32),
            pltpu.VMEM((HID, BR), F32),
            pltpu.VMEM((3, HID, BR), F32),
            pltpu.VMEM((3, HID, BR), F32),
            pltpu.VMEM((2, HID, BR), F32),
            pltpu.VMEM((CP, HID), BF16),
            pltpu.VMEM((2, NB, 16, 128), F32),
            pltpu.VMEM((2, NB, 16, 128), F32),
            pltpu.VMEM((2, 16, 128), F32),
            pltpu.VMEM((2, NB, 16, 128), F32),
            pltpu.SemaphoreType.DMA((NB,)),
            pltpu.SemaphoreType.DMA,
            pltpu.SemaphoreType.DMA((N_SEM,)),
            pltpu.SemaphoreType.DMA((N_SEM,)),
        ],
        compiler_params=pltpu.CompilerParams(
            collective_id=0, has_side_effects=True, vmem_limit_bytes=67_043_328),
        name='gcn_step',
    )(adj_rows, feat_rows.T, w_hidden, w_output.T, labels.reshape(1, -1), train_mask.reshape(1, -1))
    loss, gwh, gwo = pl.pallas_call(
        unpack,
        out_shape=(
            jax.ShapeDtypeStruct((1, 1), F32),
            jax.ShapeDtypeStruct((FI, HID), F32),
            jax.ShapeDtypeStruct((NC, HID), F32),
        ),
        in_specs=[vmem, vmem],
        out_specs=(vmem, vmem, vmem),
        name='unpack',
    )(sums, count)
    return loss[0, 0], gwh, gwo.T


def solution(mesh):
    row_spec = P(AXIS, None)
    vec_spec = P(AXIS)
    return jax.shard_map(
        device_step, mesh=mesh,
        in_specs=(row_spec, row_spec, P(), P(), vec_spec, vec_spec, P()),
        out_specs=(P(), P(), P()), check_vma=False)
```
